256 devices in a mesh: parts: 2 (over y), row: 16 (over z), chan: 4 (over x), sub: 2 (over core).
Axes of the slice: x: 4, y: 2, z: 16, core: 2. Of those that a mesh axis runs over, the one named last changes fastest.
The devices are a block of a 4x16x16 slice.
Arguments:
- pair: bfloat16 [896, 448, 128], P(('parts', 'row', 'sub'), 'chan'), parts along dimension 0, may hold values from -6 to 6
- pair_mask: int32 [896, 448], P(('parts', 'row', 'sub'), 'chan'), parts along dimension 0, may hold values 0 or 1
- out_in_gain: float32 [128], replicated, may hold values from 0.5 to 1.5
- out_proj: bfloat16 [128, 640], replicated, may hold values from -0.5 to 0.5
- out_mid_gain: float32 [128], replicated, may hold values from 0.5 to 1.5
- out_final: bfloat16 [128, 128], replicated, may hold values from -0.5 to 0.5
- in_in_gain: float32 [128], replicated, may hold values from 0.5 to 1.5
- in_proj: bfloat16 [128, 640], replicated, may hold values from -0.5 to 0.5
- in_mid_gain: float32 [128], replicated, may hold values from 0.5 to 1.5
- in_final: bfloat16 [128, 128], replicated, may hold values from -0.5 to 0.5
Outputs:
- updated: bfloat16 [896, 448, 128], P(('parts', 'row', 'sub'), 'chan'), parts along dimension 0
The draws below stay inside these ranges and needn't reach their ends.
There are 2 independent parts, one for each index of `parts`. The reference program is written for one: setup_inputs(seed, part) draws one part's arguments, and reference() takes and returns one part's arrays. A program takes and returns all parts, laid end to end along the dimension named above; an argument that names none is the same for every part. Nothing has to cross between parts.
All inputs are finite; a program needn't handle non-finite values. No bound on the sum of `pair_mask` on one device may be relied on, other than what follows from the above.
Results may differ from the reference program's by a relative error of at most 0.014.
Values may be sent and summed in bfloat16 or wider, within the bound.
No kernel may reach another device: no remote copies, remote signals or barrier semaphores. Data moves between devices by JAX's collectives and lax.ppermute only.
A program may use at most 64 MiB of HBM per device.

```python
import jax
import jax.numpy as jnp
from jax import lax

CHANNELS = 128
HIDDEN_SIZE = 128
TOKENS = 448


def place_ends(values, own_key, least, high):
    longest = values.shape.index(max(values.shape))
    spots = []
    for shift in (0, 1):
        where = [jax.random.randint(jax.random.fold_in(own_key, axis), (), 0, length) for axis, length in enumerate(values.shape)]
        where[longest] = (where[longest] + shift) % values.shape[longest]
        spots.append(tuple(where))
    return values.at[spots[0]].set(least).at[spots[1]].set(high)


def level_of(stream_key, shape, shards, low, top_value):
    def one(axis_at, blocks):
        heights = jax.random.uniform(jax.random.fold_in(jax.random.fold_in(stream_key, 6), axis_at), (blocks,), jnp.float32, low / len(shards), top_value / len(shards))
        return jnp.repeat(jnp.exp(heights), shape[axis_at] // blocks).reshape((-1,) + (1,) * (len(shape) - axis_at - 1))

    loudness = one(*shards[0])
    for cut in shards[1:]:
        loudness = loudness * one(*cut)
    return loudness


def normal_values(stream_key, shape, spread, reach, shards=(), dtype=jnp.bfloat16):
    level = level_of(stream_key, shape, shards, -0.22, 0.18) if shards else 1.0
    entries = jax.random.normal(stream_key, shape, jnp.float32) * spread * level
    return jnp.minimum(jnp.maximum(entries, -reach), reach).astype(dtype)


def setup_inputs(seed: int = 0, part: int = 0) -> dict:
    key_of = jax.random.split(jax.random.key(seed), 11)
    own_keys = jax.random.split(jax.random.fold_in(key_of[10], part), 11)
    return {
        "pair": normal_values(own_keys[0], (TOKENS, TOKENS, CHANNELS), 1.0, 6.0, ((0, 32), (1, 4))),
        "pair_mask": place_ends((jax.random.randint(own_keys[1], (TOKENS, TOKENS), 0, 4) < 3).astype(jnp.int32), jax.random.fold_in(own_keys[1], 1), 0, 1),
        "out_in_gain": jnp.clip(jax.random.uniform(key_of[2], (CHANNELS,), jnp.float32, 0.5, 1.5), 0.5, 1.5),
        "out_proj": normal_values(key_of[3], (CHANNELS, 4 * HIDDEN_SIZE + CHANNELS), CHANNELS ** -0.5, 0.5),
        "out_mid_gain": jnp.clip(jax.random.uniform(key_of[4], (HIDDEN_SIZE,), jnp.float32, 0.5, 1.5), 0.5, 1.5),
        "out_final": normal_values(key_of[5], (HIDDEN_SIZE, CHANNELS), HIDDEN_SIZE ** -0.5, 0.5),
        "in_in_gain": jnp.clip(jax.random.uniform(key_of[6], (CHANNELS,), jnp.float32, 0.5, 1.5), 0.5, 1.5),
        "in_proj": normal_values(key_of[7], (CHANNELS, 4 * HIDDEN_SIZE + CHANNELS), CHANNELS ** -0.5, 0.5),
        "in_mid_gain": jnp.clip(jax.random.uniform(key_of[8], (HIDDEN_SIZE,), jnp.float32, 0.5, 1.5), 0.5, 1.5),
        "in_final": normal_values(key_of[9], (HIDDEN_SIZE, CHANNELS), HIDDEN_SIZE ** -0.5, 0.5),
    }


def norm_last(values, gain):
    mean = lax.optimization_barrier(jnp.mean(values, axis=-1, keepdims=True))
    var = lax.optimization_barrier(jnp.mean((values - mean) ** 2, axis=-1, keepdims=True))
    return (values - mean) / jnp.sqrt(var + 1e-05) * gain

def triangle(pair, pair_mask, in_gain, proj, mid_gain, final, incoming):
    normed = norm_last(pair.astype(jnp.float32), in_gain).astype(jnp.bfloat16)
    slabs = jnp.dot(normed, proj[:, :4 * HIDDEN_SIZE], preferred_element_type=jnp.float32)
    keep = pair_mask.astype(jnp.float32)[:, :, None]
    left = (jax.nn.sigmoid(slabs[:, :, :HIDDEN_SIZE]) * slabs[:, :, HIDDEN_SIZE:2 * HIDDEN_SIZE] * keep).astype(jnp.bfloat16)
    right = (jax.nn.sigmoid(slabs[:, :, 2 * HIDDEN_SIZE:3 * HIDDEN_SIZE]) * slabs[:, :, 3 * HIDDEN_SIZE:] * keep).astype(jnp.bfloat16)
    gate = jax.nn.sigmoid(jnp.dot(normed, proj[:, 4 * HIDDEN_SIZE:], preferred_element_type=jnp.float32))
    left_c = jnp.moveaxis(left, 2, 0).astype(jnp.float32)
    right_c = jnp.moveaxis(right, 2, 0).astype(jnp.float32)
    if incoming:
        prod = jnp.einsum('cki,ckj->cij', left_c, right_c)
    else:
        prod = jnp.einsum('cik,cjk->cij', left_c, right_c)
    normed_mid = norm_last(jnp.moveaxis(prod, 0, 2), mid_gain).astype(jnp.bfloat16)
    update = gate * jnp.dot(normed_mid, final, preferred_element_type=jnp.float32)
    return (pair.astype(jnp.float32) + update).astype(jnp.bfloat16)

def reference(pair, pair_mask, out_in_gain, out_proj, out_mid_gain, out_final, in_in_gain, in_proj, in_mid_gain, in_final):
    middle = triangle(pair, pair_mask, out_in_gain, out_proj, out_mid_gain, out_final, False)
    return triangle(middle, pair_mask, in_in_gain, in_proj, in_mid_gain, in_final, True)
```

```python
import jax
import jax.numpy as jnp
from jax import lax
from jax.sharding import PartitionSpec as P

GROUP = ("chan", "row", "sub")


def norm(values, gain, axis):
    mean = jnp.mean(values, axis=axis, keepdims=True)
    var = jnp.mean((values - mean) ** 2, axis=axis, keepdims=True)
    return (values - mean) / jnp.sqrt(var + 1e-05) * gain


def exchange(values):
    return lax.all_to_all(values, GROUP, split_axis=0, concat_axis=0, tiled=True)


def slabs(pairs, keep, in_gain, proj):
    channels = pairs.shape[1]
    hidden = (proj.shape[1] - channels) // 4
    normed = norm(pairs.astype(jnp.float32), in_gain, 1).astype(jnp.bfloat16)
    raw = jnp.einsum("de,pd->ep", proj[:, : 4 * hidden], normed, preferred_element_type=jnp.float32)
    left = jax.nn.sigmoid(raw[:hidden]) * raw[hidden : 2 * hidden] * keep[None]
    right = jax.nn.sigmoid(raw[2 * hidden : 3 * hidden]) * raw[3 * hidden :] * keep[None]
    gate = jax.nn.sigmoid(
        jnp.dot(normed, proj[:, 4 * hidden :], preferred_element_type=jnp.float32)
    )
    return jnp.stack([left.astype(jnp.bfloat16), right.astype(jnp.bfloat16)], 1), gate


def update(pairs, keep, in_gain, proj, mid_gain, final, incoming, rows, cols, chans):
    both, gate = slabs(pairs, keep, in_gain, proj)
    got = exchange(both)
    size = got.shape[0]
    planes = got.reshape(chans, size // chans, 2, rows, cols)
    planes = planes.transpose(2, 1, 3, 0, 4).reshape(2, size // chans * rows, chans * cols)
    product = jnp.einsum(
        "ki,kj->ij" if incoming else "ik,jk->ij",
        planes[0],
        planes[1],
        preferred_element_type=jnp.float32,
    ).astype(jnp.bfloat16)
    parts = product.reshape(size // chans, rows, chans, cols).transpose(2, 0, 1, 3)
    whole = exchange(parts.reshape(size, 2, rows * cols // 2)).reshape(size, rows * cols)
    normed = norm(whole.astype(jnp.float32), mid_gain[:, None], 0).astype(jnp.bfloat16)
    change = jnp.einsum("cp,cd->pd", normed, final, preferred_element_type=jnp.float32)
    return (pairs.astype(jnp.float32) + gate * change).astype(jnp.bfloat16)


def solution(mesh):
    chans = mesh.shape["chan"]

    def shards(
        pair,
        pair_mask,
        out_in_gain,
        out_proj,
        out_mid_gain,
        out_final,
        in_in_gain,
        in_proj,
        in_mid_gain,
        in_final,
    ):
        rows, cols, channels = pair.shape
        pairs = pair.reshape(rows * cols, channels)
        keep = pair_mask.astype(jnp.float32).reshape(rows * cols)
        middle = update(
            pairs, keep, out_in_gain, out_proj, out_mid_gain, out_final, False, rows, cols, chans
        )
        updated = update(
            middle, keep, in_in_gain, in_proj, in_mid_gain, in_final, True, rows, cols, chans
        )
        return updated.reshape(rows, cols, channels)

    placed = (
        P(("parts", "row", "sub"), "chan", None),
        P(("parts", "row", "sub"), "chan"),
    ) + (P(),) * 8
    return jax.shard_map(
        shards,
        mesh=mesh,
        in_specs=placed,
        out_specs=P(("parts", "row", "sub"), "chan", None),
        check_vma=False,
    )
```

```python
import jax
import jax.numpy as jnp
from jax import lax
from jax.experimental import pallas as pl
from jax.experimental.pallas import tpu as pltpu
from jax.sharding import PartitionSpec as P

GROUP = ("row", "sub", "chan")


def exchange(values):
    return lax.all_to_all(values, GROUP, split_axis=0, concat_axis=0, tiled=True)


def norm(values, gain, axis):
    mean = jnp.mean(values, axis=axis, keepdims=True)
    centred = values - mean
    var = jnp.mean(centred * centred, axis=axis, keepdims=True)
    return centred * lax.rsqrt(var + 1e-05) * gain


def turned(proj):
    return proj.astype(jnp.float32).T.astype(jnp.bfloat16)


def project_tile(pairs, keep, in_gain, slab_proj, gate_proj):
    normed = norm(pairs, in_gain, 1).astype(jnp.bfloat16)
    raw = lax.dot_general(
        slab_proj, normed, (((1,), (1,)), ((), ())), preferred_element_type=jnp.float32
    )
    hidden = raw.shape[0] // 4
    left = jax.nn.sigmoid(raw[:hidden]) * raw[hidden : 2 * hidden] * keep
    right = jax.nn.sigmoid(raw[2 * hidden : 3 * hidden]) * raw[3 * hidden :] * keep
    gate = jax.nn.sigmoid(
        lax.dot_general(
            normed, gate_proj, (((1,), (0,)), ((), ())), preferred_element_type=jnp.float32
        )
    )
    return left.astype(jnp.bfloat16), right.astype(jnp.bfloat16), gate


def finish_tile(pairs, gate, product, mid_gain, final):
    normed = norm(product, mid_gain, 0).astype(jnp.bfloat16)
    change = lax.dot_general(
        normed, final, (((0,), (0,)), ((), ())), preferred_element_type=jnp.float32
    )
    return (pairs + gate * change).astype(jnp.bfloat16)


def tiles(count, half):
    out = []
    for h, size in enumerate((half, count - half)):
        cut = (size // 128 + 1) // 2 * 128
        for start, stop in ((0, cut), (cut, size)):
            out.append((h, slice(start, stop), slice(h * half + start, h * half + stop)))
    return out


def first_kernel(half, pair, mask, in_gain, proj, both, gate, keep):
    rows, cols = mask.shape
    hidden = both.shape[0]
    for r in range(rows):
        keep[:, r * cols : (r + 1) * cols] = mask[r : r + 1, :].astype(jnp.float32)
    slab_proj = turned(proj[:, : 4 * hidden])
    gate_proj = proj[:, 4 * hidden :]
    for _, _, at in tiles(pair.shape[0], half):
        left, right, gated = project_tile(
            pair[at, :].astype(jnp.float32), keep[:, at], in_gain[:, :], slab_proj, gate_proj
        )
        both[:, 0, at] = left
        both[:, 1, at] = right
        gate[at, :] = gated


def middle_kernel(
    pair, keep, gate_in, product, mid_gain, final, in_gain, proj, both, gate, middle
):
    hidden = both.shape[0]
    slab_proj = turned(proj[:, : 4 * hidden])
    gate_proj = proj[:, 4 * hidden :]
    for h, lanes, at in tiles(pair.shape[0], product.shape[2]):
        new = finish_tile(
            pair[at, :].astype(jnp.float32),
            gate_in[at, :],
            product[:, h, lanes].astype(jnp.float32),
            mid_gain[:, :],
            final[:, :],
        )
        middle[at, :] = new
        left, right, gated = project_tile(
            new.astype(jnp.float32), keep[:, at], in_gain[:, :], slab_proj, gate_proj
        )
        both[:, 0, at] = left
        both[:, 1, at] = right
        gate[at, :] = gated


def last_kernel(pair, gate_in, product, mid_gain, final, updated):
    for h, lanes, at in tiles(pair.shape[0], product.shape[2]):
        updated[at, :] = finish_tile(
            pair[at, :].astype(jnp.float32),
            gate_in[at, :],
            product[:, h, lanes].astype(jnp.float32),
            mid_gain[:, :],
            final[:, :],
        )


def call(kernel, outs, *args):
    whole = pl.BlockSpec(memory_space=pltpu.VMEM)
    return pl.pallas_call(
        kernel,
        out_shape=[jax.ShapeDtypeStruct(shape, dtype) for shape, dtype in outs],
        in_specs=[whole] * len(args),
        out_specs=[whole] * len(outs),
    )(*args)


def products(both, incoming, rows, cols, chans):
    got = exchange(both)
    size = got.shape[0]
    planes = got.reshape(size // chans, chans, 2, rows, cols)
    planes = planes.transpose(2, 0, 3, 1, 4).reshape(2, size // chans * rows, chans * cols)
    product = jnp.einsum(
        "ki,kj->ij" if incoming else "ik,jk->ij",
        planes[0],
        planes[1],
        preferred_element_type=jnp.float32,
    ).astype(jnp.bfloat16)
    parts = product.reshape(size // chans, rows, chans, cols).transpose(0, 2, 1, 3)
    tall = half_rows(rows)
    parts = jnp.pad(parts, ((0, 0), (0, 0), (0, 2 * tall - rows), (0, 0)))
    return exchange(parts.reshape(size, 2, tall * cols))


def half_rows(rows):
    return (rows + 15) // 16 * 8


def solution(mesh):
    chans = mesh.shape["chan"]

    def shards(
        pair,
        pair_mask,
        out_in_gain,
        out_proj,
        out_mid_gain,
        out_final,
        in_in_gain,
        in_proj,
        in_mid_gain,
        in_final,
    ):
        rows, cols, channels = pair.shape
        count = rows * cols
        hidden = out_final.shape[0]
        half = half_rows(rows) * cols
        pairs = pair.reshape(count, channels)
        slab_out = ((hidden, 2, count), jnp.bfloat16)
        gate_out = ((count, channels), jnp.float32)
        pair_out = ((count, channels), jnp.bfloat16)
        keep_out = ((1, count), jnp.float32)
        both, gate, keep = call(
            lambda *refs: first_kernel(half, *refs),
            [slab_out, gate_out, keep_out],
            pairs,
            pair_mask,
            out_in_gain[None],
            out_proj,
        )
        product = products(both, False, rows, cols, chans)
        both, gate, middle = call(
            middle_kernel,
            [slab_out, gate_out, pair_out],
            pairs,
            keep,
            gate,
            product,
            out_mid_gain[:, None],
            out_final,
            in_in_gain[None],
            in_proj,
        )
        product = products(both, True, rows, cols, chans)
        (updated,) = call(
            last_kernel, [pair_out], middle, gate, product, in_mid_gain[:, None], in_final
        )
        return updated.reshape(rows, cols, channels)

    placed = (
        P(("parts", "row", "sub"), "chan", None),
        P(("parts", "row", "sub"), "chan"),
    ) + (P(),) * 8
    return jax.shard_map(
        shards,
        mesh=mesh,
        in_specs=placed,
        out_specs=P(("parts", "row", "sub"), "chan", None),
        check_vma=False,
    )
```

```python
import jax
import jax.numpy as jnp
from jax import lax
from jax.experimental import pallas as pl
from jax.experimental.pallas import tpu as pltpu
from jax.sharding import PartitionSpec as P

GROUP = ("row", "sub", "chan")


def exchange(values):
    return lax.all_to_all(values, GROUP, split_axis=0, concat_axis=0, tiled=True)


def norm(values, gain, axis):
    mean = jnp.mean(values, axis=axis, keepdims=True)
    centred = values - mean
    var = jnp.mean(centred * centred, axis=axis, keepdims=True)
    return centred * lax.rsqrt(var + 1e-05) * gain


def turned(proj):
    return proj.astype(jnp.float32).T.astype(jnp.bfloat16)


def project_tile(pairs, keep, in_gain, slab_proj, gate_proj):
    normed = norm(pairs, in_gain, 1).astype(jnp.bfloat16)
    raw = lax.dot_general(
        slab_proj, normed, (((1,), (1,)), ((), ())), preferred_element_type=jnp.float32
    )
    hidden = raw.shape[0] // 4
    left = jax.nn.sigmoid(raw[:hidden]) * raw[hidden : 2 * hidden] * keep
    right = jax.nn.sigmoid(raw[2 * hidden : 3 * hidden]) * raw[3 * hidden :] * keep
    gate = jax.nn.sigmoid(
        lax.dot_general(
            normed, gate_proj, (((1,), (0,)), ((), ())), preferred_element_type=jnp.float32
        )
    )
    return left.astype(jnp.bfloat16), right.astype(jnp.bfloat16), gate


def column(gain):
    size = gain.shape[1]
    return jnp.broadcast_to(gain, (size, size)).T[:, :1]


def finish_tile(pairs, gate, product, mid_gain, final):
    normed = norm(product, mid_gain, 0).astype(jnp.bfloat16)
    change = lax.dot_general(
        normed, final, (((0,), (0,)), ((), ())), preferred_element_type=jnp.float32
    )
    return (pairs + gate * change).astype(jnp.bfloat16)


def tiles(count, half):
    out = []
    for h, size in enumerate((half, count - half)):
        cut = (size // 128 + 1) // 2 * 128
        for start, stop in ((0, cut), (cut, size)):
            out.append((h, slice(start, stop), slice(h * half + start, h * half + stop)))
    return out


def first_kernel(half, pair, mask, in_gain, proj, both, gate, keep):
    rows, cols = mask.shape
    hidden = both.shape[0]
    for r in range(rows):
        keep[:, r * cols : (r + 1) * cols] = mask[r : r + 1, :].astype(jnp.float32)
    slab_proj = turned(proj[:, : 4 * hidden])
    gate_proj = proj[:, 4 * hidden :]
    for _, _, at in tiles(pair.shape[0], half):
        left, right, gated = project_tile(
            pair[at, :].astype(jnp.float32), keep[:, at], in_gain[:, :], slab_proj, gate_proj
        )
        both[:, 0, at] = left
        both[:, 1, at] = right
        gate[at, :] = gated


def middle_kernel(
    pair, keep, gate_in, product, mid_gain, final, in_gain, proj, both, gate, middle
):
    hidden = both.shape[0]
    slab_proj = turned(proj[:, : 4 * hidden])
    gate_proj = proj[:, 4 * hidden :]
    gain = column(mid_gain[:, :])
    for h, lanes, at in tiles(pair.shape[0], product.shape[2]):
        new = finish_tile(
            pair[at, :].astype(jnp.float32),
            gate_in[at, :],
            product[:, h, lanes].astype(jnp.float32),
            gain,
            final[:, :],
        )
        middle[at, :] = new
        left, right, gated = project_tile(
            new.astype(jnp.float32), keep[:, at], in_gain[:, :], slab_proj, gate_proj
        )
        both[:, 0, at] = left
        both[:, 1, at] = right
        gate[at, :] = gated


def last_kernel(pair, gate_in, product, mid_gain, final, updated):
    gain = column(mid_gain[:, :])
    for h, lanes, at in tiles(pair.shape[0], product.shape[2]):
        updated[at, :] = finish_tile(
            pair[at, :].astype(jnp.float32),
            gate_in[at, :],
            product[:, h, lanes].astype(jnp.float32),
            gain,
            final[:, :],
        )


def call(kernel, outs, *args):
    whole = pl.BlockSpec(memory_space=pltpu.VMEM)
    return pl.pallas_call(
        kernel,
        out_shape=[jax.ShapeDtypeStruct(shape, dtype) for shape, dtype in outs],
        in_specs=[whole] * len(args),
        out_specs=[whole] * len(outs),
    )(*args)


def products(both, incoming, rows, cols, chans):
    got = exchange(both)
    size = got.shape[0]
    planes = got.reshape(size // chans, chans, 2, rows, cols)
    planes = planes.transpose(2, 0, 3, 1, 4).reshape(2, size // chans * rows, chans * cols)
    product = jnp.einsum(
        "ki,kj->ij" if incoming else "ik,jk->ij",
        planes[0],
        planes[1],
        preferred_element_type=jnp.float32,
    ).astype(jnp.bfloat16)
    parts = product.reshape(size // chans, rows, chans, cols).transpose(0, 2, 1, 3)
    tall = half_rows(rows)
    parts = jnp.pad(parts, ((0, 0), (0, 0), (0, 2 * tall - rows), (0, 0)))
    return exchange(parts.reshape(size, 2, tall * cols))


def half_rows(rows):
    return (rows + 15) // 16 * 8


def solution(mesh):
    chans = mesh.shape["chan"]

    def shards(
        pair,
        pair_mask,
        out_in_gain,
        out_proj,
        out_mid_gain,
        out_final,
        in_in_gain,
        in_proj,
        in_mid_gain,
        in_final,
    ):
        rows, cols, channels = pair.shape
        count = rows * cols
        hidden = out_final.shape[0]
        half = half_rows(rows) * cols
        pairs = pair.reshape(count, channels)
        slab_out = ((hidden, 2, count), jnp.bfloat16)
        gate_out = ((count, channels), jnp.float32)
        pair_out = ((count, channels), jnp.bfloat16)
        keep_out = ((1, count), jnp.float32)
        both, gate, keep = call(
            lambda *refs: first_kernel(half, *refs),
            [slab_out, gate_out, keep_out],
            pairs,
            pair_mask,
            out_in_gain[None],
            out_proj,
        )
        product = products(both, False, rows, cols, chans)
        both, gate, middle = call(
            middle_kernel,
            [slab_out, gate_out, pair_out],
            pairs,
            keep,
            gate,
            product,
            out_mid_gain[None],
            out_final,
            in_in_gain[None],
            in_proj,
        )
        product = products(both, True, rows, cols, chans)
        (updated,) = call(
            last_kernel, [pair_out], middle, gate, product, in_mid_gain[None], in_final
        )
        return updated.reshape(rows, cols, channels)

    placed = (
        P(("parts", "row", "sub"), "chan", None),
        P(("parts", "row", "sub"), "chan"),
    ) + (P(),) * 8
    return jax.shard_map(
        shards,
        mesh=mesh,
        in_specs=placed,
        out_specs=P(("parts", "row", "sub"), "chan", None),
        check_vma=False,
    )
```

```python
import jax
import jax.numpy as jnp
from jax import lax
from jax.experimental import pallas as pl
from jax.experimental.pallas import tpu as pltpu
from jax.sharding import PartitionSpec as P

GROUP = ("row", "chan", "sub")


def exchange(values):
    return lax.all_to_all(values, GROUP, split_axis=0, concat_axis=0, tiled=True)


def norm(values, gain, axis):
    mean = jnp.mean(values, axis=axis, keepdims=True)
    centred = values - mean
    var = jnp.mean(centred * centred, axis=axis, keepdims=True)
    return centred * lax.rsqrt(var + 1e-05) * gain


def turned(proj):
    return proj.astype(jnp.float32).T.astype(jnp.bfloat16)


def project_tile(pairs, keep, in_gain, slab_proj, gate_proj):
    normed = norm(pairs, in_gain, 1).astype(jnp.bfloat16)
    raw = lax.dot_general(
        slab_proj, normed, (((1,), (1,)), ((), ())), preferred_element_type=jnp.float32
    )
    hidden = raw.shape[0] // 4
    left = jax.nn.sigmoid(raw[:hidden]) * raw[hidden : 2 * hidden] * keep
    right = jax.nn.sigmoid(raw[2 * hidden : 3 * hidden]) * raw[3 * hidden :] * keep
    gate = jax.nn.sigmoid(
        lax.dot_general(
            normed, gate_proj, (((1,), (0,)), ((), ())), preferred_element_type=jnp.float32
        )
    )
    return left.astype(jnp.bfloat16), right.astype(jnp.bfloat16), gate


def column(gain):
    size = gain.shape[1]
    return jnp.broadcast_to(gain, (size, size)).T[:, :1]


def finish_tile(pairs, gate, product, mid_gain, final):
    normed = norm(product, mid_gain, 0).astype(jnp.bfloat16)
    change = lax.dot_general(
        normed, final, (((0,), (0,)), ((), ())), preferred_element_type=jnp.float32
    )
    return (pairs + gate * change).astype(jnp.bfloat16)


def tiles(count, half):
    out = []
    for h, size in enumerate((half, count - half)):
        cut = (size // 128 + 1) // 2 * 128
        for start, stop in ((0, cut), (cut, size)):
            out.append((h, slice(start, stop), slice(h * half + start, h * half + stop)))
    return out


def first_kernel(half, pair, mask, in_gain, proj, both, gate, keep):
    rows, cols = mask.shape
    hidden = both.shape[0]
    for r in range(rows):
        keep[:, r * cols : (r + 1) * cols] = mask[r : r + 1, :].astype(jnp.float32)
    slab_proj = turned(proj[:, : 4 * hidden])
    gate_proj = proj[:, 4 * hidden :]
    for _, _, at in tiles(pair.shape[0], half):
        left, right, gated = project_tile(
            pair[at, :].astype(jnp.float32), keep[:, at], in_gain[:, :], slab_proj, gate_proj
        )
        both[:, 0, at] = left
        both[:, 1, at] = right
        gate[at, :] = gated


def middle_kernel(
    pair, keep, gate_in, product, mid_gain, final, in_gain, proj, both, gate, middle
):
    hidden = both.shape[0]
    slab_proj = turned(proj[:, : 4 * hidden])
    gate_proj = proj[:, 4 * hidden :]
    gain = column(mid_gain[:, :])
    for h, lanes, at in tiles(pair.shape[0], product.shape[2]):
        new = finish_tile(
            pair[at, :].astype(jnp.float32),
            gate_in[at, :],
            product[:, h, lanes].astype(jnp.float32),
            gain,
            final[:, :],
        )
        middle[at, :] = new
        left, right, gated = project_tile(
            new.astype(jnp.float32), keep[:, at], in_gain[:, :], slab_proj, gate_proj
        )
        both[:, 0, at] = left
        both[:, 1, at] = right
        gate[at, :] = gated


def last_kernel(pair, gate_in, product, mid_gain, final, updated):
    gain = column(mid_gain[:, :])
    for h, lanes, at in tiles(pair.shape[0], product.shape[2]):
        updated[at, :] = finish_tile(
            pair[at, :].astype(jnp.float32),
            gate_in[at, :],
            product[:, h, lanes].astype(jnp.float32),
            gain,
            final[:, :],
        )


def call(kernel, outs, *args):
    whole = pl.BlockSpec(memory_space=pltpu.VMEM)
    return pl.pallas_call(
        kernel,
        out_shape=[jax.ShapeDtypeStruct(shape, dtype) for shape, dtype in outs],
        in_specs=[whole] * len(args),
        out_specs=[whole] * len(outs),
    )(*args)


def products(both, incoming, rows, cols, chans, subs):
    got = exchange(both)
    size = got.shape[0]
    planes = got.reshape(size // chans // subs, chans, subs, 2, rows, cols)
    planes = planes.transpose(3, 0, 2, 4, 1, 5).reshape(2, size // chans * rows, chans * cols)
    product = jnp.einsum(
        "ki,kj->ij" if incoming else "ik,jk->ij",
        planes[0],
        planes[1],
        preferred_element_type=jnp.float32,
    ).astype(jnp.bfloat16)
    parts = product.reshape(size // chans // subs, subs, rows, chans, cols)
    parts = parts.transpose(0, 3, 1, 2, 4).reshape(size // subs, subs, rows, cols)
    tall = half_rows(rows)
    parts = jnp.pad(parts, ((0, 0), (0, 0), (0, 2 * tall - rows), (0, 0)))
    return exchange(parts.reshape(size, 2, tall * cols))


def half_rows(rows):
    return (rows + 15) // 16 * 8


def solution(mesh):
    chans, subs = mesh.shape["chan"], mesh.shape["sub"]

    def shards(
        pair,
        pair_mask,
        out_in_gain,
        out_proj,
        out_mid_gain,
        out_final,
        in_in_gain,
        in_proj,
        in_mid_gain,
        in_final,
    ):
        rows, cols, channels = pair.shape
        count = rows * cols
        hidden = out_final.shape[0]
        half = half_rows(rows) * cols
        pairs = pair.reshape(count, channels)
        slab_out = ((hidden, 2, count), jnp.bfloat16)
        gate_out = ((count, channels), jnp.float32)
        pair_out = ((count, channels), jnp.bfloat16)
        keep_out = ((1, count), jnp.float32)
        both, gate, keep = call(
            lambda *refs: first_kernel(half, *refs),
            [slab_out, gate_out, keep_out],
            pairs,
            pair_mask,
            out_in_gain[None],
            out_proj,
        )
        product = products(both, False, rows, cols, chans, subs)
        both, gate, middle = call(
            middle_kernel,
            [slab_out, gate_out, pair_out],
            pairs,
            keep,
            gate,
            product,
            out_mid_gain[None],
            out_final,
            in_in_gain[None],
            in_proj,
        )
        product = products(both, True, rows, cols, chans, subs)
        (updated,) = call(
            last_kernel, [pair_out], middle, gate, product, in_mid_gain[None], in_final
        )
        return updated.reshape(rows, cols, channels)

    placed = (
        P(("parts", "row", "sub"), "chan", None),
        P(("parts", "row", "sub"), "chan"),
    ) + (P(),) * 8
    return jax.shard_map(
        shards,
        mesh=mesh,
        in_specs=placed,
        out_specs=P(("parts", "row", "sub"), "chan", None),
        check_vma=False,
    )
```
